256 devices in a mesh: gx: 8 (over z), gy: 32 (over x, y, core).
Axes of the slice: x: 4, y: 4, z: 8, core: 2. Of those that a mesh axis runs over, the one named last changes fastest.
Arguments:
- blocks: bfloat16 [2048, 8, 256, 256], P(('gx', 'gy')), may hold values from -0.1875 to 0.1875
- block_cols: int32 [2048, 8], P(('gx', 'gy')), may hold values from 0 to 23, as said below
- live_blocks: int32 [2048], P(('gx', 'gy')), may hold values from 1 to 8
- send_rows: int32 [256, 4, 4], P(('gx', 'gy')), may hold values from 0 to 7, as said below
- start: float32 [2048, 64, 256], P(('gx', 'gy')), may hold values from -6 to 6
- sketch: float32 [64, 2048, 256], P(None, ('gx', 'gy')), may hold values from -0.0009765625 to 0.0009765625
Outputs:
- basis: float32 [4, 2048, 64, 256], P(None, ('gx', 'gy'))
- factor: float32 [4, 4, 64], replicated
The draws below stay inside these ranges and needn't reach their ends.
Inputs may be any that keep to these rules, and one draw needn't show every extreme that they name: block_cols[i, 0] is block row i itself (i % 8 in the owner's numbering); only the first live_blocks[i] entries of a row are used. `send_rows`: the 4 entries of one device and direction are distinct.
All inputs are finite; a program needn't handle non-finite values.
Results may differ from the reference program's by a relative error of at most 0.0036.
Values may be sent and summed in bfloat16 or wider, within the bound.
No kernel may reach another device: no remote copies, remote signals or barrier semaphores. Data moves between devices by JAX's collectives and lax.ppermute only.
A program may use at most 64 MiB of HBM per device.

```python
import jax
import jax.numpy as jnp
from jax import lax

BS = 256
RB = 8
KB = 8
NRHS = 64
SK = 64
STEPS = 3
H = 4
NBR = 2048
NROWS = 524288
N_GX = 8
N_GY = 32
DEVICES = 256


def draw_block_cols(key, part):
    own_rows = (jnp.arange(NBR, dtype=jnp.int32) % RB)[:, None]
    others = jax.random.randint(jax.random.fold_in(key, 11), (NBR, KB - 1), 0, RB + 4 * H, dtype=jnp.int32)
    return jnp.concatenate([own_rows, others], axis=1).astype(jnp.int32)


def draw_send_rows(key, part):
    keys = jax.random.split(jax.random.fold_in(key, 7), DEVICES * 4)
    orders = jax.vmap(lambda single: jax.random.permutation(single, RB))(keys)
    return orders[:, :H].reshape(DEVICES, 4, H).astype(jnp.int32)


def plant(array, own_key, low, top_value):
    extent = array.shape
    place = [jax.random.randint(jax.random.fold_in(own_key, axis), (), 0, extent[axis]) for axis in range(len(extent))]
    array = array.at[tuple(place)].set(low)
    longest = extent.index(max(extent))
    place[longest] = (place[longest] + 1) % extent[longest]
    return array.at[tuple(place)].set(top_value)


def steps_of(stream_key, extent, cuts, low, largest):
    def one(position, blocks):
        steps = jax.random.uniform(jax.random.fold_in(jax.random.fold_in(stream_key, 6), position), (blocks,), jnp.float32, low / len(cuts), largest / len(cuts))
        return jnp.repeat(jnp.exp(steps), extent[position] // blocks).reshape((-1,) + (1,) * (len(extent) - position - 1))

    factor_of = one(*cuts[0])
    for cut in cuts[1:]:
        factor_of = factor_of * one(*cut)
    return factor_of


def scatter_about(rng, extent, width, most, cuts=(), kind=jnp.bfloat16):
    entries = width * jax.random.normal(rng, extent, jnp.float32)
    if cuts:
        entries = entries * steps_of(rng, extent, cuts, -0.22, 0.18)
    return jnp.clip(entries, -most, most).astype(kind)


def setup_inputs(seed: int = 0) -> dict:
    key_list = jax.random.split(jax.random.key(seed), 7)
    return {
        "blocks": scatter_about(key_list[0], (NBR, KB, BS, BS), (BS * KB // 2) ** -0.5, 0.1875, ((0, 256),)),
        "block_cols": draw_block_cols(jax.random.fold_in(key_list[6], 71), 0),
        "live_blocks": plant(jax.random.randint(key_list[2], (NBR,), 1, KB + 1), jax.random.fold_in(key_list[2], 1), 1, KB).astype(jnp.int32),
        "send_rows": draw_send_rows(jax.random.fold_in(key_list[6], 71), 0),
        "start": scatter_about(key_list[4], (NBR, NRHS, BS), 1.0, 6.0, ((0, 256),), jnp.float32),
        "sketch": scatter_about(key_list[5], (SK, NBR, BS), (SK * NROWS) ** -0.5, 0.0009765625, ((1, 256),), jnp.float32),
    }


def global_columns(block_cols, send_rows):
    owner = (jnp.arange(NBR, dtype=jnp.int32) // RB)[:, None]
    outer = owner // N_GY
    inner = owner % N_GY
    ghost = block_cols - RB
    direct = jnp.clip(ghost // H, 0, 3).astype(jnp.int32)
    within = (ghost % H).astype(jnp.int32)
    step_gy = jnp.where(direct == 0, -1, jnp.where(direct == 1, 1, 0))
    step_gx = jnp.where(direct == 2, -1, jnp.where(direct == 3, 1, 0))
    source = ((outer + step_gx) % N_GX * N_GY + (inner + step_gy) % N_GY).astype(jnp.int32)
    remote = source * RB + send_rows[source, direct, within]
    return jnp.where(block_cols < RB, owner * RB + block_cols, remote).astype(jnp.int32)

def power_step(vectors, columns, weights, blocks):
    rounded = vectors.astype(jnp.bfloat16)

    def one_device(pieces):
        cols, weight, block = pieces
        picked = rounded[cols].astype(jnp.float32) * weight[:, :, None, None]
        return jnp.einsum('ikrb,ikbc->irc', picked, block.astype(jnp.float32))
    result = lax.map(one_device, (columns.reshape(DEVICES, RB, KB), weights.reshape(DEVICES, RB, KB), blocks.reshape(DEVICES, RB, KB, BS, BS)))
    return result.reshape(NBR, NRHS, BS)

def orthogonalize(sketched):
    count = sketched.shape[0]
    columns = []
    factor = jnp.zeros((count, count, sketched.shape[2]), jnp.float32)
    for column in range(count):
        residue = sketched[column]
        for earlier in range(column):
            coefficient = lax.optimization_barrier(jnp.sum(columns[earlier] * sketched[column], axis=0))
            factor = factor.at[earlier, column].set(coefficient)
            residue = residue - coefficient[None, :] * columns[earlier]
        length = jnp.sqrt(lax.optimization_barrier(jnp.sum(residue * residue, axis=0)) + 1e-06)
        factor = factor.at[column, column].set(length)
        columns.append(residue / length[None, :])
    return factor

def reference(blocks, block_cols, live_blocks, send_rows, start, sketch):
    columns = global_columns(block_cols, send_rows)
    weights = (jnp.arange(KB, dtype=jnp.int32)[None, :] < live_blocks[:, None]).astype(jnp.float32)
    vectors = [start]
    for section in range(STEPS):
        vectors.append(power_step(vectors[-1], columns, weights, blocks))
    sketched = jnp.stack([jnp.einsum('sib,irb->sr', sketch, vector, precision=lax.Precision.HIGHEST) for vector in vectors])
    factor = orthogonalize(sketched)
    result = []
    for column in range(STEPS + 1):
        accum = vectors[column]
        for earlier in range(column):
            accum = accum - factor[earlier, column][None, :, None] * result[earlier]
        result.append(accum / factor[column, column][None, :, None])
    return (jnp.stack(result), factor)
```

```python
import jax
import jax.numpy as jnp
from jax import lax
from jax.experimental import pallas as pl
from jax.experimental.pallas import tpu as pltpu
from jax.sharding import Mesh
from jax.sharding import PartitionSpec as P

STEPS = 3
GY = ("y0", "y1", "core")
GX_GY = ("gx", "y0", "y1", "core")
F32, BF16 = jnp.float32, jnp.bfloat16
VMEM = pl.BlockSpec(memory_space=pltpu.VMEM)
SMEM = pl.BlockSpec(memory_space=pltpu.SMEM)


def call(kernel, name, ins, outs, scratch=(), flops=0, nbytes=0, out_specs=None):
    return pl.pallas_call(
        kernel,
        name=name,
        in_specs=ins,
        out_specs=out_specs or [VMEM] * len(outs),
        out_shape=outs,
        scratch_shapes=scratch,
        cost_estimate=pl.CostEstimate(flops=flops, bytes_accessed=nbytes, transcendentals=0),
        compiler_params=pltpu.CompilerParams(vmem_limit_bytes=24 << 20),
    )


def parities():
    return lax.axis_index("core"), lax.rem(lax.axis_index("gx"), 2)


def directions(side, layer):
    received = (1 - side, side, 3 - layer, 2 + layer)
    sent = (side, 1 - side, 2 + layer, 3 - layer)
    return received, sent


def fill_messages(send, rows, outs, side, layer):
    _, sent = directions(side, layer)
    for out, direction in zip(outs, sent, strict=True):
        for j in range(out.shape[0]):
            out[j] = rows[send[0, direction, j]]


def first_kernel(send, start, x_out, *outs):
    side, layer = parities()
    x_out[...] = start[...].astype(BF16)
    fill_messages(send, x_out, outs, side, layer)


def place_rows(x, received, src, side, layer):
    count = x.shape[0]
    width = received[0].shape[0]
    src[:count] = x[...]
    numbers, _ = directions(side, layer)
    for ref, direction in zip(received, numbers, strict=True):
        src[pl.ds(count + direction * width, width)] = ref[...]
    src[count + 4 * width] = jnp.zeros(src.shape[1:], src.dtype)


def product_of_row(i, cols, live, src, blocks):
    slots, dead = cols.shape[1], src.shape[0] - 1
    picked = [src[jnp.where(k < live[i], cols[i, k], dead)] for k in range(slots)]
    tall = blocks[i].reshape(slots * blocks.shape[2], blocks.shape[3])
    return jnp.dot(jnp.concatenate(picked, axis=1), tall, preferred_element_type=F32)


def step_kernel(cols, live, send, x, ra, rb, rc, rd, blocks, v_out, x_out, oa, ob, oc, od, src):
    side, layer = parities()
    place_rows(x, (ra, rb, rc, rd), src, side, layer)
    for i in range(x.shape[0]):
        v = product_of_row(i, cols, live, src, blocks)
        v_out[i] = v
        x_out[i] = v.astype(BF16)
    fill_messages(send, x_out, (oa, ob, oc, od), side, layer)


def halves(v):
    high = v.astype(BF16)
    return high, (v - high.astype(F32)).astype(BF16)


def sketched(v, high, low):
    left, right = [], []
    for i in range(v.shape[0]):
        v_high, v_low = halves(v[i])
        left += [v_high, v_low, v_high]
        right += [high[i], high[i], low[i]]
    return lax.dot_general(
        jnp.concatenate(left, axis=1),
        jnp.concatenate(right, axis=1),
        (((1,), (1,)), ((), ())),
        preferred_element_type=F32,
    )


def prepare_kernel(sketch, start, high, low, w_out):
    for i in range(start.shape[0]):
        high[i], low[i] = halves(sketch[:, i, :])
    w_out[...] = sketched(start, high, low)


def sketch_kernel(v, high, low, w_out):
    w_out[...] = sketched(v, high, low)


def last_kernel(cols, live, x, ra, rb, rc, rd, blocks, high, low, w0, w1, w2, v_out, w_out, src):
    side, layer = parities()
    place_rows(x, (ra, rb, rc, rd), src, side, layer)
    for i in range(x.shape[0]):
        v_out[i] = product_of_row(i, cols, live, src, blocks)
    w3 = sketched(v_out, high, low)
    w_out[0] = jnp.concatenate([w0[...], w1[...]], axis=1)
    w_out[1] = jnp.concatenate([w2[...], w3], axis=1)


def final_kernel(v0, v1, v2, v3, w, basis, factor_out, out, sems):
    count = 4
    size = w.shape[2] // 2
    sums = [w[s // 2][:, (s % 2) * size : (s % 2 + 1) * size] for s in range(count)]
    columns, factor, inverse = [], {}, []
    for s in range(count):
        residue = sums[s]
        for m in range(s):
            factor[m, s] = jnp.sum(columns[m] * sums[s], axis=1, keepdims=True)
            residue = residue - factor[m, s] * columns[m]
        factor[s, s] = jnp.sqrt(jnp.sum(residue * residue, axis=1, keepdims=True) + 1e-06)
        inverse.append(1.0 / factor[s, s])
        columns.append(residue * inverse[s])
    copies = []
    for s, v in enumerate((v0, v1, v2, v3)):
        for i in range(v.shape[0]):
            total = v[i]
            for m in range(s):
                total = total - factor[m, s] * out[m, i]
            out[s, i] = total * inverse[s]
        copies.append(pltpu.make_async_copy(out.at[s], basis.at[s], sems.at[s]))
        copies[-1].start()
    lane = lax.broadcasted_iota(jnp.int32, (w.shape[1], 128), 1)
    table = jnp.zeros((w.shape[1], 128), F32)
    for (m, s), value in factor.items():
        table = table + jnp.where(lane == m * count + s, value, 0.0)
    table = table.T
    for m in range(count):
        factor_out[m] = table[m * count : (m + 1) * count]
    for copy in copies:
        copy.wait()


def swaps(count, offset):
    pairs = []
    for i in range(offset, count + offset, 2):
        a, b = i % count, (i + 1) % count
        pairs += [(a, b), (b, a)]
    return pairs


def exchange(messages):
    oa, ob, oc, od = messages
    gy, gx = lax.axis_size(GY), lax.axis_size("gx")
    rd = lax.ppermute(od, "gx", swaps(gx, 1))
    rc = lax.ppermute(oc, "gx", swaps(gx, 0))
    rb = lax.ppermute(ob, GY, swaps(gy, 1))
    ra = lax.ppermute(oa, GY, swaps(gy, 0))
    return ra, rb, rc, rd


def shifted_sum(x, axis):
    count = lax.axis_size(axis)
    parts = [lax.ppermute(x, axis, [(i, (i + k) % count) for i in range(count)]) for k in range(1, count)]
    return sum(parts, x)


def doubled_sum(x, axis):
    count = lax.axis_size(axis)
    k = 1
    while k < count:
        x = x + lax.ppermute(x, axis, [(i, i ^ k) for i in range(count)])
        k *= 2
    return x


def summed(x):
    x = doubled_sum(x, "core")
    x = shifted_sum(x, "y1")
    x = shifted_sum(x, "y0")
    return doubled_sum(x, "gx")


def on_device(blocks, block_cols, live_blocks, send_rows, start, sketch):
    rows, slots, size, _ = blocks.shape
    rhs = start.shape[1]
    width = send_rows.shape[2]
    count = sketch.shape[0]
    vector = jax.ShapeDtypeStruct(start.shape, F32)
    rounded = jax.ShapeDtypeStruct(start.shape, BF16)
    message = jax.ShapeDtypeStruct((width, rhs, size), BF16)
    part = jax.ShapeDtypeStruct((rhs, count), F32)
    src = pltpu.VMEM((rows + 4 * width + 1, rhs, size), BF16)
    flops = 2 * rows * slots * rhs * size * size
    sketch_flops = 6 * rows * rhs * size * count

    x, *messages = call(
        first_kernel, "first", [SMEM, VMEM], [rounded] + [message] * 4, flops=1 << 20, nbytes=1 << 20
    )(send_rows, start)
    received = exchange(messages)
    high, low, w0 = call(
        prepare_kernel, "prepare", [VMEM] * 2, [rounded] * 2 + [part], flops=sketch_flops, nbytes=1 << 20
    )(sketch, start)
    step = call(
        step_kernel,
        "step",
        [SMEM] * 3 + [VMEM] * 6,
        [vector, rounded] + [message] * 4,
        [src],
        flops=flops,
        nbytes=blocks.size * 2,
    )
    sketch_of = call(sketch_kernel, "sketch", [VMEM] * 3, [part], flops=sketch_flops, nbytes=1 << 20)
    v1, x, *messages = step(block_cols, live_blocks, send_rows, x, *received, blocks)
    received = exchange(messages)
    (w1,) = sketch_of(v1, high, low)
    v2, x, *messages = step(block_cols, live_blocks, send_rows, x, *received, blocks)
    received = exchange(messages)
    (w2,) = sketch_of(v2, high, low)
    v3, w = call(
        last_kernel,
        "last",
        [SMEM] * 2 + [VMEM] * 11,
        [vector, jax.ShapeDtypeStruct((2, rhs, 2 * count), F32)],
        [src],
        flops=flops + sketch_flops,
        nbytes=blocks.size * 2,
    )(block_cols, live_blocks, x, *received, blocks, high, low, w0, w1, w2)
    w = summed(w)
    basis, factor = call(
        final_kernel,
        "final",
        [VMEM] * 5,
        [
            jax.ShapeDtypeStruct((STEPS + 1, *start.shape), F32),
            jax.ShapeDtypeStruct((STEPS + 1, STEPS + 1, rhs), F32),
        ],
        [pltpu.VMEM((STEPS + 1, *start.shape), F32), pltpu.SemaphoreType.DMA((STEPS + 1,))],
        flops=1 << 22,
        nbytes=1 << 22,
        out_specs=[pl.BlockSpec(memory_space=pl.ANY), VMEM],
    )(start, v1, v2, v3, w)
    return basis, factor


def solution(mesh):
    split = Mesh(mesh.devices.reshape(mesh.shape["gx"], 4, 4, 2), GX_GY)
    return jax.shard_map(
        on_device,
        mesh=split,
        in_specs=(
            P(GX_GY, None, None, None),
            P(GX_GY, None),
            P(GX_GY),
            P(GX_GY, None, None),
            P(GX_GY, None, None),
            P(None, GX_GY, None),
        ),
        out_specs=(P(None, GX_GY, None, None), P()),
        check_vma=False,
    )
```

```python
import jax
import jax.numpy as jnp
from jax import lax
from jax.experimental import pallas as pl
from jax.experimental.pallas import tpu as pltpu
from jax.sharding import Mesh
from jax.sharding import PartitionSpec as P

STEPS = 3
GY = ("y0", "y1", "core")
GX_GY = ("gx", "y0", "y1", "core")
F32, BF16 = jnp.float32, jnp.bfloat16
VMEM = pl.BlockSpec(memory_space=pltpu.VMEM)
SMEM = pl.BlockSpec(memory_space=pltpu.SMEM)
HBM = pl.BlockSpec(memory_space=pltpu.HBM)


def call(kernel, name, ins, outs, scratch=(), flops=0, nbytes=0, out_specs=None):
    return pl.pallas_call(
        kernel,
        name=name,
        in_specs=ins,
        out_specs=out_specs or [VMEM] * len(outs),
        out_shape=outs,
        scratch_shapes=scratch,
        cost_estimate=pl.CostEstimate(flops=flops, bytes_accessed=nbytes, transcendentals=0),
        compiler_params=pltpu.CompilerParams(vmem_limit_bytes=24 << 20),
    )


def in_hbm(x):
    return pltpu.with_memory_space_constraint(x, pltpu.HBM)


def parities():
    return lax.axis_index("core"), lax.rem(lax.axis_index("gx"), 2)


def directions(side, layer):
    received = (1 - side, side, 3 - layer, 2 + layer)
    sent = (side, 1 - side, 2 + layer, 3 - layer)
    return received, sent


def fill_messages(send, rows, outs, side, layer):
    _, sent = directions(side, layer)
    for out, direction in zip(outs, sent, strict=True):
        for j in range(out.shape[0]):
            out[j] = rows[send[0, direction, j]]


def copy_all(pairs, sems):
    copies = [pltpu.make_async_copy(source, target, sems.at[n]) for n, (source, target) in enumerate(pairs)]
    for copy in copies:
        copy.start()
    return copies


def first_kernel(send_hbm, start_hbm, v_out, send_out, x_out, oa, ob, oc, od, send, sems):
    copies = copy_all(((send_hbm, send), (start_hbm, v_out), (send_hbm, send_out)), sems)
    side, layer = parities()
    for copy in copies:
        copy.wait()
    x_out[...] = v_out[...].astype(BF16)
    fill_messages(send, x_out, (oa, ob, oc, od), side, layer)


def place_rows(x, received, src, side, layer):
    count = x.shape[0]
    width = received[0].shape[0]
    src[:count] = x[...]
    numbers, _ = directions(side, layer)
    for ref, direction in zip(received, numbers, strict=True):
        src[pl.ds(count + direction * width, width)] = ref[...]
    src[count + 4 * width] = jnp.zeros(src.shape[1:], src.dtype)


def product_of_row(i, cols, live, src, blocks):
    slots, dead = cols.shape[1], src.shape[0] - 1
    picked = [src[jnp.where(k < live[i], cols[i, k], dead)] for k in range(slots)]
    tall = blocks[i].reshape(slots * blocks.shape[2], blocks.shape[3])
    return jnp.dot(jnp.concatenate(picked, axis=1), tall, preferred_element_type=F32)


def step_kernel(cols, live, send, x, rd, rc, ra, rb, blocks, v_out, x_out, oa, ob, oc, od, src):
    side, layer = parities()
    place_rows(x, (ra, rb, rc, rd), src, side, layer)
    for i in range(x.shape[0]):
        v = product_of_row(i, cols, live, src, blocks)
        v_out[i] = v
        x_out[i] = v.astype(BF16)
    fill_messages(send, x_out, (oa, ob, oc, od), side, layer)


def halves(v):
    high = v.astype(BF16)
    return high, (v - high.astype(F32)).astype(BF16)


def sketched(v, high, low):
    left, right = [], []
    for i in range(v.shape[0]):
        v_high, v_low = halves(v[i])
        left += [v_high, v_low, v_high]
        right += [high[i], high[i], low[i]]
    return lax.dot_general(
        jnp.concatenate(left, axis=1),
        jnp.concatenate(right, axis=1),
        (((1,), (1,)), ((), ())),
        preferred_element_type=F32,
    )


def prepare_kernel(
    blocks_hbm, sketch_hbm, cols_hbm, live_hbm, start, blocks, cols, live, high, low, w_out, sketch, sems
):
    rows = start.shape[0]
    pairs = [(sketch_hbm, sketch)]
    pairs += [(blocks_hbm.at[i], blocks.at[i]) for i in range(rows)]
    pairs += [(cols_hbm, cols), (live_hbm, live)]
    copies = copy_all(pairs, sems)
    copies[0].wait()
    for i in range(rows):
        high[i], low[i] = halves(sketch[:, i, :])
    w_out[...] = sketched(start, high, low)
    for copy in copies[1:]:
        copy.wait()


def sketch_kernel(v, high, low, w_out):
    w_out[...] = sketched(v, high, low)


def spread_kernel(low_row, high_row, cols, live, high, blocks, *refs):
    z = refs[-1]
    dead = z.shape[0] - 1
    if low_row == 0:
        z[...] = jnp.zeros(z.shape, z.dtype)
    else:
        z[...] = refs[0][...]
    for i in range(low_row, high_row):
        for k in range(cols.shape[1]):
            column = jnp.where(k < live[i], cols[i, k], dead)
            z[column] += lax.dot_general(
                high[i], blocks[i, k], (((1,), (1,)), ((), ())), preferred_element_type=F32
            )


def against(rows, z_rows):
    left, right = [], []
    for row, z_row in zip(rows, z_rows, strict=True):
        left += [row, row]
        right += list(halves(z_row))
    return lax.dot_general(
        jnp.concatenate(left, axis=1),
        jnp.concatenate(right, axis=1),
        (((1,), (1,)), ((), ())),
        preferred_element_type=F32,
    )


def own_kernel(x, z, w_out):
    own = range(x.shape[0])
    w_out[...] = against([x[e] for e in own], [z[e] for e in own])


def gather_kernel(rd, rc, ra, rb, z, w0, w1, w2, own, w_out):
    side, layer = parities()
    numbers, _ = directions(side, layer)
    width = ra.shape[0]
    count = z.shape[0] - 1 - 4 * width
    rows, z_rows = [], []
    for ref, direction in zip((ra, rb, rc, rd), numbers, strict=True):
        rows += [ref[j] for j in range(width)]
        z_rows += [z[count + direction * width + j] for j in range(width)]
    w_out[0] = jnp.concatenate([w0[...], w1[...]], axis=1)
    w_out[1] = jnp.concatenate([w2[...], own[...] + against(rows, z_rows)], axis=1)


def last_kernel(cols, live, x, rd, rc, ra, rb, blocks, v_out, src):
    side, layer = parities()
    place_rows(x, (ra, rb, rc, rd), src, side, layer)
    for i in range(x.shape[0]):
        v_out[i] = product_of_row(i, cols, live, src, blocks)


def final_kernel(v0, v1, v2, v3, w, basis, factor_out, out, sems):
    count = 4
    size = w.shape[2] // 2
    sums = [w[s // 2][:, (s % 2) * size : (s % 2 + 1) * size] for s in range(count)]
    columns, inverse, factor, copies = [], [], {}, []
    vectors = (v0, v1, v2, v3)

    def add_column(s):
        residue = sums[s]
        for m in range(s):
            factor[m, s] = jnp.sum(columns[m] * sums[s], axis=1, keepdims=True)
            residue = residue - factor[m, s] * columns[m]
        factor[s, s] = jnp.sqrt(jnp.sum(residue * residue, axis=1, keepdims=True) + 1e-06)
        inverse.append(1.0 / factor[s, s])
        columns.append(residue * inverse[s])

    def write_basis(s):
        for i in range(v0.shape[0]):
            total = vectors[s][i]
            for m in range(s):
                total = total - factor[m, s] * out[m, i]
            out[s, i] = total * inverse[s]
        copies.append(pltpu.make_async_copy(out.at[s], basis.at[s], sems.at[s]))
        copies[-1].start()

    add_column(0)
    for s in range(1, count):
        add_column(s)
        write_basis(s - 1)
    write_basis(count - 1)
    lane = lax.broadcasted_iota(jnp.int32, (w.shape[1], 128), 1)
    table = jnp.zeros((w.shape[1], 128), F32)
    for (m, s), value in factor.items():
        table = table + jnp.where(lane == m * count + s, value, 0.0)
    table = table.T
    for m in range(count):
        factor_out[m] = table[m * count : (m + 1) * count]
    for copy in copies:
        copy.wait()


def swaps(count, offset):
    pairs = []
    for i in range(offset, count + offset, 2):
        a, b = i % count, (i + 1) % count
        pairs += [(a, b), (b, a)]
    return pairs


def exchange(messages):
    oa, ob, oc, od = messages
    gy, gx = lax.axis_size(GY), lax.axis_size("gx")
    rd = lax.ppermute(od, "gx", swaps(gx, 1))
    rc = lax.ppermute(oc, "gx", swaps(gx, 0))
    ra = lax.ppermute(oa, GY, swaps(gy, 0))
    rb = lax.ppermute(ob, GY, swaps(gy, 1))
    return rd, rc, ra, rb


def rounded_to(x):
    return lax.reduce_precision(x, 8, 7)


def ring_sum(x, axis):
    count = lax.axis_size(axis)
    x = rounded_to(x)
    sent = x.astype(BF16)
    parts = [lax.ppermute(sent, axis, [(i, i ^ k) for i in range(count)]).astype(F32) for k in range(1, count)]
    return (parts[0] + parts[2]) + (x + parts[1])


def doubled_sum(x, axis):
    count = lax.axis_size(axis)
    k = 1
    while k < count:
        x = rounded_to(x)
        x = x + lax.ppermute(x.astype(BF16), axis, [(i, i ^ k) for i in range(count)]).astype(F32)
        k *= 2
    return x


def summed(x):
    x = x + lax.ppermute(x, "core", [(0, 1), (1, 0)])
    x = ring_sum(x, "y1")
    x = ring_sum(x, "y0")
    return doubled_sum(x, "gx")


def on_device(blocks, block_cols, live_blocks, send_rows, start, sketch):
    rows, slots, size, _ = blocks.shape
    rhs = start.shape[1]
    width = send_rows.shape[2]
    count = sketch.shape[0]
    vector = jax.ShapeDtypeStruct(start.shape, F32)
    rounded = jax.ShapeDtypeStruct(start.shape, BF16)
    message = jax.ShapeDtypeStruct((width, rhs, size), BF16)
    part = jax.ShapeDtypeStruct((rhs, count), F32)
    src = pltpu.VMEM((rows + 4 * width + 1, rhs, size), BF16)
    flops = 2 * rows * slots * rhs * size * size
    sketch_flops = 6 * rows * rhs * size * count

    v0, send, x, *messages = call(
        first_kernel,
        "first",
        [HBM] * 2,
        [vector, jax.ShapeDtypeStruct(send_rows.shape, jnp.int32), rounded] + [message] * 4,
        [pltpu.SMEM(send_rows.shape, jnp.int32), pltpu.SemaphoreType.DMA((3,))],
        flops=1 << 20,
        nbytes=1 << 20,
    )(in_hbm(send_rows), in_hbm(start))
    received = exchange(messages)
    here, cols, live, high, low, w0 = call(
        prepare_kernel,
        "prepare",
        [HBM] * 4 + [VMEM],
        [
            jax.ShapeDtypeStruct(blocks.shape, BF16),
            jax.ShapeDtypeStruct(block_cols.shape, jnp.int32),
            jax.ShapeDtypeStruct(live_blocks.shape, jnp.int32),
            rounded,
            rounded,
            part,
        ],
        [pltpu.VMEM(sketch.shape, F32), pltpu.SemaphoreType.DMA((rows + 3,))],
        flops=sketch_flops,
        nbytes=blocks.size * 2,
    )(in_hbm(blocks), in_hbm(sketch), in_hbm(block_cols), in_hbm(live_blocks), v0)

    def step(x, received, *earlier):
        inputs = (cols, live, send, x, *received, here)

        def kernel(*refs):
            step_kernel(*refs[: len(inputs)], *refs[len(inputs) + len(earlier) :])

        return call(
            kernel,
            "step",
            [SMEM] * 3 + [VMEM] * (6 + len(earlier)),
            [vector, rounded] + [message] * 4,
            [src],
            flops=flops,
            nbytes=blocks.size * 2,
        )(*inputs, *earlier)

    sketch_of = call(sketch_kernel, "sketch", [VMEM] * 3, [part], flops=sketch_flops, nbytes=1 << 20)
    v1, x, *messages = step(x, received)
    received = exchange(messages)
    (w1,) = sketch_of(v1, high, low)
    half = rows // 2
    table = jax.ShapeDtypeStruct((src.shape[0], count, size), F32)

    def spread(name, low_row, high_row, extra):
        return call(
            lambda *refs: spread_kernel(low_row, high_row, *refs),
            name,
            [SMEM] * 2 + [VMEM] * (2 + extra),
            [table],
            flops=flops,
            nbytes=blocks.size,
        )

    (z,) = spread("spread", 0, half, 0)(cols, live, high, here)
    v2, x, *messages = step(x, received, z, w1)
    received = exchange(messages)
    (w2,) = sketch_of(v2, high, low)
    (z,) = spread("respread", half, rows, 1)(cols, live, high, here, z)
    (own,) = call(own_kernel, "own", [VMEM] * 2, [part], flops=sketch_flops, nbytes=1 << 20)(x, z)
    (w,) = call(
        gather_kernel,
        "gather",
        [VMEM] * 9,
        [jax.ShapeDtypeStruct((2, rhs, 2 * count), F32)],
        flops=sketch_flops,
        nbytes=1 << 20,
    )(*received, z, w0, w1, w2, own)
    (v3,) = call(
        last_kernel,
        "last",
        [SMEM] * 2 + [VMEM] * 6,
        [vector],
        [src],
        flops=flops,
        nbytes=blocks.size * 2,
    )(cols, live, x, *received, here)
    w = summed(w)
    basis, factor = call(
        final_kernel,
        "final",
        [VMEM] * 5,
        [
            jax.ShapeDtypeStruct((STEPS + 1, *start.shape), F32),
            jax.ShapeDtypeStruct((STEPS + 1, STEPS + 1, rhs), F32),
        ],
        [pltpu.VMEM((STEPS + 1, *start.shape), F32), pltpu.SemaphoreType.DMA((STEPS + 1,))],
        flops=1 << 22,
        nbytes=1 << 22,
        out_specs=[pl.BlockSpec(memory_space=pl.ANY), VMEM],
    )(v0, v1, v2, v3, w)
    return basis, factor


def solution(mesh):
    split = Mesh(mesh.devices.reshape(mesh.shape["gx"], 4, 4, 2), GX_GY)
    return jax.shard_map(
        on_device,
        mesh=split,
        in_specs=(
            P(GX_GY, None, None, None),
            P(GX_GY, None),
            P(GX_GY),
            P(GX_GY, None, None),
            P(GX_GY, None, None),
            P(None, GX_GY, None),
        ),
        out_specs=(P(None, GX_GY, None, None), P()),
        check_vma=False,
    )
```

```python
import jax
import jax.numpy as jnp
from jax import lax
from jax.experimental import pallas as pl
from jax.experimental.pallas import tpu as pltpu
from jax.sharding import Mesh
from jax.sharding import PartitionSpec as P

STEPS = 3
GY = ("y0", "y1", "core")
GX_GY = ("gx", "y0", "y1", "core")
F32, BF16 = jnp.float32, jnp.bfloat16
VMEM = pl.BlockSpec(memory_space=pltpu.VMEM)
SMEM = pl.BlockSpec(memory_space=pltpu.SMEM)
HBM = pl.BlockSpec(memory_space=pltpu.HBM)


def call(kernel, name, ins, outs, scratch=(), flops=0, nbytes=0, out_specs=None):
    return pl.pallas_call(
        kernel,
        name=name,
        in_specs=ins,
        out_specs=out_specs or [VMEM] * len(outs),
        out_shape=outs,
        scratch_shapes=scratch,
        cost_estimate=pl.CostEstimate(flops=flops, bytes_accessed=nbytes, transcendentals=0),
        compiler_params=pltpu.CompilerParams(vmem_limit_bytes=24 << 20),
    )


def in_hbm(x):
    return pltpu.with_memory_space_constraint(x, pltpu.HBM)


def parities():
    return lax.axis_index("core"), lax.rem(lax.axis_index("gx"), 2)


def directions(side, layer):
    received = (1 - side, side, 3 - layer, 2 + layer)
    sent = (side, 1 - side, 2 + layer, 3 - layer)
    return received, sent


def fill_messages(send, rows, outs, side, layer):
    _, sent = directions(side, layer)
    for out, direction in zip(outs, sent, strict=True):
        for j in range(out.shape[0]):
            out[j] = rows[send[0, direction, j]]


def copy_all(pairs, sems):
    copies = [pltpu.make_async_copy(source, target, sems.at[n]) for n, (source, target) in enumerate(pairs)]
    for copy in copies:
        copy.start()
    return copies


def first_kernel(send_hbm, start_hbm, v_out, send_out, x_out, oa, ob, oc, od, send, sems):
    copies = copy_all(((send_hbm, send), (start_hbm, v_out), (send_hbm, send_out)), sems)
    side, layer = parities()
    for copy in copies:
        copy.wait()
    x_out[...] = v_out[...].astype(BF16)
    fill_messages(send, x_out, (oa, ob, oc, od), side, layer)


def place_rows(x, received, src, side, layer):
    count = x.shape[0]
    width = received[0].shape[0]
    src[:count] = x[...]
    numbers, _ = directions(side, layer)
    for ref, direction in zip(received, numbers, strict=True):
        src[pl.ds(count + direction * width, width)] = ref[...]
    src[count + 4 * width] = jnp.zeros(src.shape[1:], src.dtype)


def product_of_row(i, cols, live, src, blocks):
    slots, dead = cols.shape[1], src.shape[0] - 1
    picked = [src[jnp.where(k < live[i], cols[i, k], dead)] for k in range(slots)]
    tall = blocks[i].reshape(slots * blocks.shape[2], blocks.shape[3])
    return jnp.dot(jnp.concatenate(picked, axis=1), tall, preferred_element_type=F32)


def step_kernel(cols, live, send, x, rb, rd, rc, ra, blocks, v_out, x_out, oa, ob, oc, od, src):
    side, layer = parities()
    place_rows(x, (ra, rb, rc, rd), src, side, layer)
    for i in range(x.shape[0]):
        v = product_of_row(i, cols, live, src, blocks)
        v_out[i] = v
        x_out[i] = v.astype(BF16)
    fill_messages(send, x_out, (oa, ob, oc, od), side, layer)


def halves(v):
    high = v.astype(BF16)
    return high, (v - high.astype(F32)).astype(BF16)


def sketched(v, high, low):
    left, right = [], []
    for i in range(v.shape[0]):
        v_high, v_low = halves(v[i])
        left += [v_high, v_low, v_high]
        right += [high[i], high[i], low[i]]
    return lax.dot_general(
        jnp.concatenate(left, axis=1),
        jnp.concatenate(right, axis=1),
        (((1,), (1,)), ((), ())),
        preferred_element_type=F32,
    )


def prepare_kernel(
    blocks_hbm, sketch_hbm, cols_hbm, live_hbm, start, blocks, cols, live, high, low, w_out, sketch, sems
):
    rows = start.shape[0]
    pairs = [(sketch_hbm, sketch)]
    pairs += [(blocks_hbm.at[i], blocks.at[i]) for i in range(rows)]
    pairs += [(cols_hbm, cols), (live_hbm, live)]
    copies = copy_all(pairs, sems)
    copies[0].wait()
    for i in range(rows):
        high[i], low[i] = halves(sketch[:, i, :])
    w_out[...] = sketched(start, high, low)
    for copy in copies[1:]:
        copy.wait()


def sketch_kernel(v, high, low, w_out):
    w_out[...] = sketched(v, high, low)


def spread_kernel(low_row, high_row, cols, live, high, blocks, *refs):
    z = refs[-1]
    dead = z.shape[0] - 1
    if low_row == 0:
        z[...] = jnp.zeros(z.shape, z.dtype)
    else:
        z[...] = refs[0][...]
    for i in range(low_row, high_row):
        for k in range(cols.shape[1]):
            column = jnp.where(k < live[i], cols[i, k], dead)
            z[column] += lax.dot_general(
                high[i], blocks[i, k], (((1,), (1,)), ((), ())), preferred_element_type=F32
            )


def against(rows, z_rows):
    left, right = [], []
    for row, z_row in zip(rows, z_rows, strict=True):
        left += [row, row]
        right += list(halves(z_row))
    return lax.dot_general(
        jnp.concatenate(left, axis=1),
        jnp.concatenate(right, axis=1),
        (((1,), (1,)), ((), ())),
        preferred_element_type=F32,
    )


def own_kernel(x, z, w_out):
    own = range(x.shape[0])
    w_out[...] = against([x[e] for e in own], [z[e] for e in own])


def gather_kernel(rb, rd, rc, ra, z, w0, w1, w2, own, w_out):
    side, layer = parities()
    numbers, _ = directions(side, layer)
    width = ra.shape[0]
    count = z.shape[0] - 1 - 4 * width
    rows, z_rows = [], []
    for ref, direction in zip((ra, rb, rc, rd), numbers, strict=True):
        rows += [ref[j] for j in range(width)]
        z_rows += [z[count + direction * width + j] for j in range(width)]
    w_out[0] = jnp.concatenate([w0[...], w1[...]], axis=1)
    w_out[1] = jnp.concatenate([w2[...], own[...] + against(rows, z_rows)], axis=1)


def last_kernel(cols, live, x, rb, rd, rc, ra, blocks, v_out, src):
    side, layer = parities()
    place_rows(x, (ra, rb, rc, rd), src, side, layer)
    for i in range(x.shape[0]):
        v_out[i] = product_of_row(i, cols, live, src, blocks)


def final_kernel(v0, v1, v2, v3, w, basis, factor_out, out, sems):
    count = 4
    size = w.shape[2] // 2
    sums = [w[s // 2][:, (s % 2) * size : (s % 2 + 1) * size] for s in range(count)]
    columns, inverse, factor, copies = [], [], {}, []
    vectors = (v0, v1, v2, v3)

    def add_column(s):
        residue = sums[s]
        for m in range(s):
            factor[m, s] = jnp.sum(columns[m] * sums[s], axis=1, keepdims=True)
            residue = residue - factor[m, s] * columns[m]
        factor[s, s] = jnp.sqrt(jnp.sum(residue * residue, axis=1, keepdims=True) + 1e-06)
        inverse.append(1.0 / factor[s, s])
        columns.append(residue * inverse[s])

    def write_basis(s):
        for i in range(v0.shape[0]):
            total = vectors[s][i]
            for m in range(s):
                total = total - factor[m, s] * out[m, i]
            out[s, i] = total * inverse[s]
        copies.append(pltpu.make_async_copy(out.at[s], basis.at[s], sems.at[s]))
        copies[-1].start()

    add_column(0)
    for s in range(1, count):
        add_column(s)
        write_basis(s - 1)
    write_basis(count - 1)
    lane = lax.broadcasted_iota(jnp.int32, (w.shape[1], 128), 1)
    table = jnp.zeros((w.shape[1], 128), F32)
    for (m, s), value in factor.items():
        table = table + jnp.where(lane == m * count + s, value, 0.0)
    table = table.T
    for m in range(count):
        factor_out[m] = table[m * count : (m + 1) * count]
    for copy in copies:
        copy.wait()


def swaps(count, offset):
    pairs = []
    for i in range(offset, count + offset, 2):
        a, b = i % count, (i + 1) % count
        pairs += [(a, b), (b, a)]
    return pairs


def exchange(messages):
    oa, ob, oc, od = messages
    gy, gx = lax.axis_size(GY), lax.axis_size("gx")
    rd = lax.ppermute(od, "gx", swaps(gx, 1))
    rc = lax.ppermute(oc, "gx", swaps(gx, 0))
    ra = lax.ppermute(oa, GY, swaps(gy, 0))
    rb = lax.ppermute(ob, GY, swaps(gy, 1))
    return rb, rd, rc, ra


def rounded_to(x):
    return lax.reduce_precision(x, 8, 7)


def four_sum(x, axes, low, high):
    count = lax.axis_size(axes)
    x = rounded_to(x)
    sent = x.astype(BF16)
    one, two, three = (
        lax.ppermute(sent, axes, [(i, i ^ bits) for i in range(count)]).astype(F32)
        for bits in (low, high, low + high)
    )
    return (one + three) + (x + two)


def summed(x):
    x = four_sum(x, ("gx", "core"), 1, 2)
    x = four_sum(x, "y1", 1, 2)
    x = four_sum(x, "y0", 1, 2)
    return four_sum(x, "gx", 2, 4)


def on_device(blocks, block_cols, live_blocks, send_rows, start, sketch):
    rows, slots, size, _ = blocks.shape
    rhs = start.shape[1]
    width = send_rows.shape[2]
    count = sketch.shape[0]
    vector = jax.ShapeDtypeStruct(start.shape, F32)
    rounded = jax.ShapeDtypeStruct(start.shape, BF16)
    message = jax.ShapeDtypeStruct((width, rhs, size), BF16)
    part = jax.ShapeDtypeStruct((rhs, count), F32)
    src = pltpu.VMEM((rows + 4 * width + 1, rhs, size), BF16)
    flops = 2 * rows * slots * rhs * size * size
    sketch_flops = 6 * rows * rhs * size * count

    v0, send, x, *messages = call(
        first_kernel,
        "first",
        [HBM] * 2,
        [vector, jax.ShapeDtypeStruct(send_rows.shape, jnp.int32), rounded] + [message] * 4,
        [pltpu.SMEM(send_rows.shape, jnp.int32), pltpu.SemaphoreType.DMA((3,))],
        flops=1 << 20,
        nbytes=1 << 20,
    )(in_hbm(send_rows), in_hbm(start))
    received = exchange(messages)
    here, cols, live, high, low, w0 = call(
        prepare_kernel,
        "prepare",
        [HBM] * 4 + [VMEM],
        [
            jax.ShapeDtypeStruct(blocks.shape, BF16),
            jax.ShapeDtypeStruct(block_cols.shape, jnp.int32),
            jax.ShapeDtypeStruct(live_blocks.shape, jnp.int32),
            rounded,
            rounded,
            part,
        ],
        [pltpu.VMEM(sketch.shape, F32), pltpu.SemaphoreType.DMA((rows + 3,))],
        flops=sketch_flops,
        nbytes=blocks.size * 2,
    )(in_hbm(blocks), in_hbm(sketch), in_hbm(block_cols), in_hbm(live_blocks), v0)

    def step(x, received, *earlier):
        inputs = (cols, live, send, x, *received, here)

        def kernel(*refs):
            step_kernel(*refs[: len(inputs)], *refs[len(inputs) + len(earlier) :])

        return call(
            kernel,
            "step",
            [SMEM] * 3 + [VMEM] * (6 + len(earlier)),
            [vector, rounded] + [message] * 4,
            [src],
            flops=flops,
            nbytes=blocks.size * 2,
        )(*inputs, *earlier)

    sketch_of = call(sketch_kernel, "sketch", [VMEM] * 3, [part], flops=sketch_flops, nbytes=1 << 20)
    v1, x, *messages = step(x, received)
    received = exchange(messages)
    (w1,) = sketch_of(v1, high, low)
    half = rows // 2
    table = jax.ShapeDtypeStruct((src.shape[0], count, size), F32)

    def spread(name, low_row, high_row, extra):
        return call(
            lambda *refs: spread_kernel(low_row, high_row, *refs),
            name,
            [SMEM] * 2 + [VMEM] * (2 + extra),
            [table],
            flops=flops,
            nbytes=blocks.size,
        )

    (z,) = spread("spread", 0, half, 0)(cols, live, high, here)
    v2, x, *messages = step(x, received, z, w1)
    received = exchange(messages)
    (w2,) = sketch_of(v2, high, low)
    (z,) = spread("respread", half, rows, 1)(cols, live, high, here, z)
    (own,) = call(own_kernel, "own", [VMEM] * 2, [part], flops=sketch_flops, nbytes=1 << 20)(x, z)
    (w,) = call(
        gather_kernel,
        "gather",
        [VMEM] * 9,
        [jax.ShapeDtypeStruct((2, rhs, 2 * count), F32)],
        flops=sketch_flops,
        nbytes=1 << 20,
    )(*received, z, w0, w1, w2, own)
    (v3,) = call(
        last_kernel,
        "last",
        [SMEM] * 2 + [VMEM] * 6,
        [vector],
        [src],
        flops=flops,
        nbytes=blocks.size * 2,
    )(cols, live, x, *received, here)
    w = summed(w)
    basis, factor = call(
        final_kernel,
        "final",
        [VMEM] * 5,
        [
            jax.ShapeDtypeStruct((STEPS + 1, *start.shape), F32),
            jax.ShapeDtypeStruct((STEPS + 1, STEPS + 1, rhs), F32),
        ],
        [pltpu.VMEM((STEPS + 1, *start.shape), F32), pltpu.SemaphoreType.DMA((STEPS + 1,))],
        flops=1 << 22,
        nbytes=1 << 22,
        out_specs=[pl.BlockSpec(memory_space=pl.ANY), VMEM],
    )(v0, v1, v2, v3, w)
    return basis, factor


def solution(mesh):
    split = Mesh(mesh.devices.reshape(mesh.shape["gx"], 4, 4, 2), GX_GY)
    return jax.shard_map(
        on_device,
        mesh=split,
        in_specs=(
            P(GX_GY, None, None, None),
            P(GX_GY, None),
            P(GX_GY),
            P(GX_GY, None, None),
            P(GX_GY, None, None),
            P(None, GX_GY, None),
        ),
        out_specs=(P(None, GX_GY, None, None), P()),
        check_vma=False,
    )
```

```python
import jax
import jax.numpy as jnp
from jax import lax
from jax.experimental import pallas as pl
from jax.experimental.pallas import tpu as pltpu
from jax.sharding import Mesh
from jax.sharding import PartitionSpec as P

STEPS = 3
GY = ("y0", "y1", "core")
GX_GY = ("gx", "y0", "y1", "core")
F32, BF16 = jnp.float32, jnp.bfloat16
VMEM = pl.BlockSpec(memory_space=pltpu.VMEM)
SMEM = pl.BlockSpec(memory_space=pltpu.SMEM)
HBM = pl.BlockSpec(memory_space=pltpu.HBM)


def call(kernel, name, ins, outs, scratch=(), flops=0, nbytes=0, out_specs=None):
    return pl.pallas_call(
        kernel,
        name=name,
        in_specs=ins,
        out_specs=out_specs or [VMEM] * len(outs),
        out_shape=outs,
        scratch_shapes=scratch,
        cost_estimate=pl.CostEstimate(flops=flops, bytes_accessed=nbytes, transcendentals=0),
        compiler_params=pltpu.CompilerParams(vmem_limit_bytes=24 << 20),
    )


def in_hbm(x):
    return pltpu.with_memory_space_constraint(x, pltpu.HBM)


def parities():
    return lax.axis_index("core"), lax.rem(lax.axis_index("gx"), 2)


def directions(side, layer):
    received = (1 - side, side, 3 - layer, 2 + layer)
    sent = (side, 1 - side, 2 + layer, 3 - layer)
    return received, sent


def fill_messages(send, rows, outs, side, layer):
    _, sent = directions(side, layer)
    for out, direction in zip(outs, sent, strict=True):
        for j in range(out.shape[0]):
            out[j] = rows[send[0, direction, j]]


def copy_all(pairs, sems):
    copies = [pltpu.make_async_copy(source, target, sems.at[n]) for n, (source, target) in enumerate(pairs)]
    for copy in copies:
        copy.start()
    return copies


def first_kernel(send_hbm, start_hbm, v_out, send_out, x_out, oa, ob, oc, od, send, sems):
    copies = copy_all(((send_hbm, send), (start_hbm, v_out), (send_hbm, send_out)), sems)
    side, layer = parities()
    for copy in copies:
        copy.wait()
    x_out[...] = v_out[...].astype(BF16)
    fill_messages(send, x_out, (oa, ob, oc, od), side, layer)


def place_rows(x, received, src, side, layer):
    count = x.shape[0]
    width = received[0].shape[0]
    src[:count] = x[...]
    numbers, _ = directions(side, layer)
    for ref, direction in zip(received, numbers, strict=True):
        src[pl.ds(count + direction * width, width)] = ref[...]
    src[count + 4 * width] = jnp.zeros(src.shape[1:], src.dtype)


def product_of_row(i, cols, live, src, blocks):
    slots, dead = cols.shape[1], src.shape[0] - 1
    picked = [src[jnp.where(k < live[i], cols[i, k], dead)] for k in range(slots)]
    tall = blocks[i].reshape(slots * blocks.shape[2], blocks.shape[3])
    return jnp.dot(jnp.concatenate(picked, axis=1), tall, preferred_element_type=F32)


def step_kernel(cols, live, send, x, rb, rc, rd, ra, blocks, v_out, x_out, oa, ob, oc, od, src):
    side, layer = parities()
    place_rows(x, (ra, rb, rc, rd), src, side, layer)
    for i in range(x.shape[0]):
        v = product_of_row(i, cols, live, src, blocks)
        v_out[i] = v
        x_out[i] = v.astype(BF16)
    fill_messages(send, x_out, (oa, ob, oc, od), side, layer)


def halves(v):
    high = v.astype(BF16)
    return high, (v - high.astype(F32)).astype(BF16)


def sketched(v, high, low):
    left, right = [], []
    for i in range(v.shape[0]):
        v_high, v_low = halves(v[i])
        left += [v_high, v_low, v_high]
        right += [high[i], high[i], low[i]]
    return lax.dot_general(
        jnp.concatenate(left, axis=1),
        jnp.concatenate(right, axis=1),
        (((1,), (1,)), ((), ())),
        preferred_element_type=F32,
    )


def prepare_kernel(
    blocks_hbm, sketch_hbm, cols_hbm, live_hbm, start, blocks, cols, live, high, low, w_out, sketch, sems
):
    rows = start.shape[0]
    pairs = [(sketch_hbm, sketch)]
    pairs += [(blocks_hbm.at[i], blocks.at[i]) for i in range(rows)]
    pairs += [(cols_hbm, cols), (live_hbm, live)]
    copies = copy_all(pairs, sems)
    copies[0].wait()
    for i in range(rows):
        high[i], low[i] = halves(sketch[:, i, :])
    w_out[...] = sketched(start, high, low)
    for copy in copies[1:]:
        copy.wait()


def sketch_kernel(v, high, low, w_out):
    w_out[...] = sketched(v, high, low)


def spread_kernel(low_row, high_row, cols, live, high, blocks, *refs):
    z = refs[-1]
    dead = z.shape[0] - 1
    if low_row == 0:
        z[...] = jnp.zeros(z.shape, z.dtype)
    else:
        z[...] = refs[0][...]
    for i in range(low_row, high_row):
        for k in range(cols.shape[1]):
            column = jnp.where(k < live[i], cols[i, k], dead)
            z[column] += lax.dot_general(
                high[i], blocks[i, k], (((1,), (1,)), ((), ())), preferred_element_type=F32
            )


def against(rows, z_rows):
    left, right = [], []
    for row, z_row in zip(rows, z_rows, strict=True):
        left += [row, row]
        right += list(halves(z_row))
    return lax.dot_general(
        jnp.concatenate(left, axis=1),
        jnp.concatenate(right, axis=1),
        (((1,), (1,)), ((), ())),
        preferred_element_type=F32,
    )


def own_kernel(x, z, w_out):
    own = range(x.shape[0])
    w_out[...] = against([x[e] for e in own], [z[e] for e in own])


def gather_kernel(rb, rc, rd, ra, z, w0, w1, w2, own, w_out):
    side, layer = parities()
    numbers, _ = directions(side, layer)
    width = ra.shape[0]
    count = z.shape[0] - 1 - 4 * width
    rows, z_rows = [], []
    for ref, direction in zip((ra, rb, rc, rd), numbers, strict=True):
        rows += [ref[j] for j in range(width)]
        z_rows += [z[count + direction * width + j] for j in range(width)]
    w_out[0] = jnp.concatenate([w0[...], w1[...]], axis=1)
    w_out[1] = jnp.concatenate([w2[...], own[...] + against(rows, z_rows)], axis=1)


def last_kernel(cols, live, x, rb, rc, rd, ra, blocks, v_out, src):
    side, layer = parities()
    place_rows(x, (ra, rb, rc, rd), src, side, layer)
    for i in range(x.shape[0]):
        v_out[i] = product_of_row(i, cols, live, src, blocks)


def final_kernel(v0, v1, v2, v3, w, basis, factor_hbm, out, factor_out, sems):
    count = 4
    size = w.shape[2] // 2
    sums = [w[s // 2][:, (s % 2) * size : (s % 2 + 1) * size] for s in range(count)]
    columns, inverse, factor, copies = [], [], {}, []
    vectors = (v0, v1, v2, v3)

    def add_column(s):
        residue = sums[s]
        for m in range(s):
            factor[m, s] = jnp.sum(columns[m] * sums[s], axis=1, keepdims=True)
            residue = residue - factor[m, s] * columns[m]
        factor[s, s] = jnp.sqrt(jnp.sum(residue * residue, axis=1, keepdims=True) + 1e-06)
        inverse.append(1.0 / factor[s, s])
        columns.append(residue * inverse[s])

    def write_basis(s):
        for i in range(v0.shape[0]):
            total = vectors[s][i]
            for m in range(s):
                total = total - factor[m, s] * out[m, i]
            out[s, i] = total * inverse[s]
        copies.append(pltpu.make_async_copy(out.at[s], basis.at[s], sems.at[s]))
        copies[-1].start()

    add_column(0)
    for s in range(1, count):
        add_column(s)
        write_basis(s - 1)
    lane = lax.broadcasted_iota(jnp.int32, (w.shape[1], 128), 1)
    table = jnp.zeros((w.shape[1], 128), F32)
    for (m, s), value in factor.items():
        table = table + jnp.where(lane == m * count + s, value, 0.0)
    table = table.T
    for m in range(count):
        factor_out[m] = table[m * count : (m + 1) * count]
    copies.append(pltpu.make_async_copy(factor_out, factor_hbm, sems.at[count]))
    copies[-1].start()
    write_basis(count - 1)
    for copy in copies:
        copy.wait()


def swaps(count, offset):
    pairs = []
    for i in range(offset, count + offset, 2):
        a, b = i % count, (i + 1) % count
        pairs += [(a, b), (b, a)]
    return pairs


def exchange(messages):
    oa, ob, oc, od = messages
    gy, gx = lax.axis_size(GY), lax.axis_size("gx")
    rd = lax.ppermute(od, "gx", swaps(gx, 1))
    rc = lax.ppermute(oc, "gx", swaps(gx, 0))
    ra = lax.ppermute(oa, GY, swaps(gy, 0))
    rb = lax.ppermute(ob, GY, swaps(gy, 1))
    return rb, rc, rd, ra


def rounded_to(x):
    return lax.reduce_precision(x, 8, 7)


def four_sum(x, axes, low, high):
    count = lax.axis_size(axes)
    x = rounded_to(x)
    sent = x.astype(BF16)
    one, two, three = (
        lax.ppermute(sent, axes, [(i, i ^ bits) for i in range(count)]).astype(F32)
        for bits in (low, high, low + high)
    )
    return (one + three) + (x + two)


def summed(x):
    x = four_sum(x, ("gx", "core"), 1, 2)
    x = four_sum(x, "y1", 1, 2)
    x = four_sum(x, "y0", 1, 2)
    return four_sum(x, "gx", 2, 4)


def on_device(blocks, block_cols, live_blocks, send_rows, start, sketch):
    rows, slots, size, _ = blocks.shape
    rhs = start.shape[1]
    width = send_rows.shape[2]
    count = sketch.shape[0]
    vector = jax.ShapeDtypeStruct(start.shape, F32)
    rounded = jax.ShapeDtypeStruct(start.shape, BF16)
    message = jax.ShapeDtypeStruct((width, rhs, size), BF16)
    part = jax.ShapeDtypeStruct((rhs, count), F32)
    src = pltpu.VMEM((rows + 4 * width + 1, rhs, size), BF16)
    flops = 2 * rows * slots * rhs * size * size
    sketch_flops = 6 * rows * rhs * size * count

    v0, send, x, *messages = call(
        first_kernel,
        "first",
        [HBM] * 2,
        [vector, jax.ShapeDtypeStruct(send_rows.shape, jnp.int32), rounded] + [message] * 4,
        [pltpu.SMEM(send_rows.shape, jnp.int32), pltpu.SemaphoreType.DMA((3,))],
        flops=1 << 20,
        nbytes=1 << 20,
    )(in_hbm(send_rows), in_hbm(start))
    received = exchange(messages)
    here, cols, live, high, low, w0 = call(
        prepare_kernel,
        "prepare",
        [HBM] * 4 + [VMEM],
        [
            jax.ShapeDtypeStruct(blocks.shape, BF16),
            jax.ShapeDtypeStruct(block_cols.shape, jnp.int32),
            jax.ShapeDtypeStruct(live_blocks.shape, jnp.int32),
            rounded,
            rounded,
            part,
        ],
        [pltpu.VMEM(sketch.shape, F32), pltpu.SemaphoreType.DMA((rows + 3,))],
        flops=sketch_flops,
        nbytes=blocks.size * 2,
    )(in_hbm(blocks), in_hbm(sketch), in_hbm(block_cols), in_hbm(live_blocks), v0)

    def step(x, received, *earlier):
        inputs = (cols, live, send, x, *received, here)

        def kernel(*refs):
            step_kernel(*refs[: len(inputs)], *refs[len(inputs) + len(earlier) :])

        return call(
            kernel,
            "step",
            [SMEM] * 3 + [VMEM] * (6 + len(earlier)),
            [vector, rounded] + [message] * 4,
            [src],
            flops=flops,
            nbytes=blocks.size * 2,
        )(*inputs, *earlier)

    sketch_of = call(sketch_kernel, "sketch", [VMEM] * 3, [part], flops=sketch_flops, nbytes=1 << 20)
    v1, x, *messages = step(x, received)
    received = exchange(messages)
    (w1,) = sketch_of(v1, high, low)
    half = rows // 2
    table = jax.ShapeDtypeStruct((src.shape[0], count, size), F32)

    def spread(name, low_row, high_row, extra):
        return call(
            lambda *refs: spread_kernel(low_row, high_row, *refs),
            name,
            [SMEM] * 2 + [VMEM] * (2 + extra),
            [table],
            flops=flops,
            nbytes=blocks.size,
        )

    (z,) = spread("spread", 0, half, 0)(cols, live, high, here)
    v2, x, *messages = step(x, received, z, w1)
    received = exchange(messages)
    (w2,) = sketch_of(v2, high, low)
    (z,) = spread("respread", half, rows, 1)(cols, live, high, here, z)
    (own,) = call(own_kernel, "own", [VMEM] * 2, [part], flops=sketch_flops, nbytes=1 << 20)(x, z)
    (w,) = call(
        gather_kernel,
        "gather",
        [VMEM] * 9,
        [jax.ShapeDtypeStruct((2, rhs, 2 * count), F32)],
        flops=sketch_flops,
        nbytes=1 << 20,
    )(*received, z, w0, w1, w2, own)
    (v3,) = call(
        last_kernel,
        "last",
        [SMEM] * 2 + [VMEM] * 6,
        [vector],
        [src],
        flops=flops,
        nbytes=blocks.size * 2,
    )(cols, live, x, *received, here)
    w = summed(w)
    basis, factor = call(
        final_kernel,
        "final",
        [VMEM] * 5,
        [
            jax.ShapeDtypeStruct((STEPS + 1, *start.shape), F32),
            jax.ShapeDtypeStruct((STEPS + 1, STEPS + 1, rhs), F32),
        ],
        [
            pltpu.VMEM((STEPS + 1, *start.shape), F32),
            pltpu.VMEM((STEPS + 1, STEPS + 1, rhs), F32),
            pltpu.SemaphoreType.DMA((STEPS + 2,)),
        ],
        flops=1 << 22,
        nbytes=1 << 22,
        out_specs=[pl.BlockSpec(memory_space=pl.ANY)] * 2,
    )(v0, v1, v2, v3, w)
    return basis, factor


def solution(mesh):
    split = Mesh(mesh.devices.reshape(mesh.shape["gx"], 4, 4, 2), GX_GY)
    return jax.shard_map(
        on_device,
        mesh=split,
        in_specs=(
            P(GX_GY, None, None, None),
            P(GX_GY, None),
            P(GX_GY),
            P(GX_GY, None, None),
            P(GX_GY, None, None),
            P(None, GX_GY, None),
        ),
        out_specs=(P(None, GX_GY, None, None), P()),
        check_vma=False,
    )
```

```python
import jax
import jax.numpy as jnp
from jax import lax
from jax.experimental import pallas as pl
from jax.experimental.pallas import tpu as pltpu
from jax.sharding import Mesh
from jax.sharding import PartitionSpec as P

STEPS = 3
GY = ("y0", "y1", "core")
GX_GY = ("gx", "y0", "y1", "core")
F32, BF16 = jnp.float32, jnp.bfloat16
VMEM = pl.BlockSpec(memory_space=pltpu.VMEM)
SMEM = pl.BlockSpec(memory_space=pltpu.SMEM)
HBM = pl.BlockSpec(memory_space=pltpu.HBM)


def call(kernel, name, ins, outs, scratch=(), flops=0, nbytes=0, out_specs=None):
    return pl.pallas_call(
        kernel,
        name=name,
        in_specs=ins,
        out_specs=out_specs or [VMEM] * len(outs),
        out_shape=outs,
        scratch_shapes=scratch,
        cost_estimate=pl.CostEstimate(flops=flops, bytes_accessed=nbytes, transcendentals=0),
        compiler_params=pltpu.CompilerParams(vmem_limit_bytes=24 << 20),
    )


def in_hbm(x):
    return pltpu.with_memory_space_constraint(x, pltpu.HBM)


def parities():
    return lax.axis_index("core"), lax.rem(lax.axis_index("gx"), 2)


def directions(side, layer):
    received = (1 - side, side, 3 - layer, 2 + layer)
    sent = (side, 1 - side, 2 + layer, 3 - layer)
    return received, sent


def fill_messages(send, rows, outs, side, layer):
    _, sent = directions(side, layer)
    for out, direction in zip(outs, sent, strict=True):
        for j in range(out.shape[0]):
            out[j] = rows[send[0, direction, j]]


def copy_all(pairs, sems):
    copies = [pltpu.make_async_copy(source, target, sems.at[n]) for n, (source, target) in enumerate(pairs)]
    for copy in copies:
        copy.start()
    return copies


def first_kernel(send_hbm, start_hbm, v_out, send_out, x_out, oa, ob, oc, od, send, sems):
    copies = copy_all(((send_hbm, send), (start_hbm, v_out), (send_hbm, send_out)), sems)
    side, layer = parities()
    for copy in copies:
        copy.wait()
    x_out[...] = v_out[...].astype(BF16)
    fill_messages(send, x_out, (oa, ob, oc, od), side, layer)


def place_rows(x, received, src, side, layer):
    count = x.shape[0]
    width = received[0].shape[0]
    src[:count] = x[...]
    numbers, _ = directions(side, layer)
    for ref, direction in zip(received, numbers, strict=True):
        src[pl.ds(count + direction * width, width)] = ref[...]
    src[count + 4 * width] = jnp.zeros(src.shape[1:], src.dtype)


def product_of_row(i, cols, live, src, blocks):
    slots, dead = cols.shape[1], src.shape[0] - 1
    picked = [src[jnp.where(k < live[i], cols[i, k], dead)] for k in range(slots)]
    tall = blocks[i].reshape(slots * blocks.shape[2], blocks.shape[3])
    return jnp.dot(jnp.concatenate(picked, axis=1), tall, preferred_element_type=F32)


def step_kernel(cols, live, send, x, rb, rc, rd, ra, blocks, v_out, x_out, oa, ob, oc, od, src):
    side, layer = parities()
    place_rows(x, (ra, rb, rc, rd), src, side, layer)
    for i in range(x.shape[0]):
        v = product_of_row(i, cols, live, src, blocks)
        v_out[i] = v
        x_out[i] = v.astype(BF16)
    fill_messages(send, x_out, (oa, ob, oc, od), side, layer)


def halves(v):
    high = v.astype(BF16)
    return high, (v - high.astype(F32)).astype(BF16)


def sketched(v, high, low):
    left, right = [], []
    for i in range(v.shape[0]):
        v_high, v_low = halves(v[i])
        left += [v_high, v_low, v_high]
        right += [high[i], high[i], low[i]]
    return lax.dot_general(
        jnp.concatenate(left, axis=1),
        jnp.concatenate(right, axis=1),
        (((1,), (1,)), ((), ())),
        preferred_element_type=F32,
    )


def prepare_kernel(
    blocks_hbm, sketch_hbm, cols_hbm, live_hbm, start, blocks, cols, live, high, low, w_out, sketch, sems
):
    rows = start.shape[0]
    pairs = [(sketch_hbm, sketch)]
    pairs += [(blocks_hbm.at[i], blocks.at[i]) for i in range(rows)]
    pairs += [(cols_hbm, cols), (live_hbm, live)]
    copies = copy_all(pairs, sems)
    copies[0].wait()
    for i in range(rows):
        high[i], low[i] = halves(sketch[:, i, :])
    w_out[...] = sketched(start, high, low)
    for copy in copies[1:]:
        copy.wait()


def sketch_kernel(v, high, low, w_out):
    w_out[...] = sketched(v, high, low)


def spread_kernel(low_row, high_row, cols, live, high, blocks, *refs):
    z = refs[-1]
    dead = z.shape[0] - 1
    if low_row == 0:
        z[...] = jnp.zeros(z.shape, z.dtype)
    else:
        z[...] = refs[0][...]
    for i in range(low_row, high_row):
        for k in range(cols.shape[1]):
            column = jnp.where(k < live[i], cols[i, k], dead)
            z[column] += lax.dot_general(
                high[i], blocks[i, k], (((1,), (1,)), ((), ())), preferred_element_type=F32
            )


def against(rows, z_halves):
    left, right = [], []
    for row, pair in zip(rows, z_halves, strict=True):
        left += [row, row]
        right += list(pair)
    return lax.dot_general(
        jnp.concatenate(left, axis=1),
        jnp.concatenate(right, axis=1),
        (((1,), (1,)), ((), ())),
        preferred_element_type=F32,
    )


def own_kernel(x, z, w_out, z_high, z_low):
    count = x.shape[0]
    w_out[...] = against([x[e] for e in range(count)], [halves(z[e]) for e in range(count)])
    for e in range(z_high.shape[0]):
        z_high[e], z_low[e] = halves(z[count + e])


def gather_kernel(rb, rc, rd, ra, z_high, z_low, w0, w1, w2, own, w_out):
    side, layer = parities()
    numbers, _ = directions(side, layer)
    width = ra.shape[0]
    rows, z_halves = [], []
    for ref, direction in zip((ra, rb, rc, rd), numbers, strict=True):
        rows += [ref[j] for j in range(width)]
        places = [direction * width + j for j in range(width)]
        z_halves += [(z_high[place], z_low[place]) for place in places]
    w_out[0] = jnp.concatenate([w0[...], w1[...]], axis=1)
    w_out[1] = jnp.concatenate([w2[...], own[...] + against(rows, z_halves)], axis=1)


def last_kernel(cols, live, x, rb, rc, rd, ra, blocks, v_out, src):
    side, layer = parities()
    place_rows(x, (ra, rb, rc, rd), src, side, layer)
    for i in range(x.shape[0]):
        v_out[i] = product_of_row(i, cols, live, src, blocks)


def final_kernel(v0, v1, v2, v3, w, basis, factor_hbm, out, factor_out, sems):
    count = 4
    size = w.shape[2] // 2
    sums = [w[s // 2][:, (s % 2) * size : (s % 2 + 1) * size] for s in range(count)]
    columns, inverse, factor, copies = [], [], {}, []
    vectors = (v0, v1, v2, v3)

    def add_column(s):
        residue = sums[s]
        for m in range(s):
            factor[m, s] = jnp.sum(columns[m] * sums[s], axis=1, keepdims=True)
            residue = residue - factor[m, s] * columns[m]
        factor[s, s] = jnp.sqrt(jnp.sum(residue * residue, axis=1, keepdims=True) + 1e-06)
        inverse.append(1.0 / factor[s, s])
        columns.append(residue * inverse[s])

    def write_basis(s):
        for i in range(v0.shape[0]):
            total = vectors[s][i]
            for m in range(s):
                total = total - factor[m, s] * out[m, i]
            out[s, i] = total * inverse[s]
        copies.append(pltpu.make_async_copy(out.at[s], basis.at[s], sems.at[s]))
        copies[-1].start()

    add_column(0)
    for s in range(1, count):
        add_column(s)
        write_basis(s - 1)
    lane = lax.broadcasted_iota(jnp.int32, (w.shape[1], 128), 1)
    table = jnp.zeros((w.shape[1], 128), F32)
    for (m, s), value in factor.items():
        table = table + jnp.where(lane == m * count + s, value, 0.0)
    table = table.T
    for m in range(count):
        factor_out[m] = table[m * count : (m + 1) * count]
    copies.append(pltpu.make_async_copy(factor_out, factor_hbm, sems.at[count]))
    copies[-1].start()
    write_basis(count - 1)
    for copy in copies:
        copy.wait()


def swaps(count, offset):
    pairs = []
    for i in range(offset, count + offset, 2):
        a, b = i % count, (i + 1) % count
        pairs += [(a, b), (b, a)]
    return pairs


def exchange(messages):
    oa, ob, oc, od = messages
    gy, gx = lax.axis_size(GY), lax.axis_size("gx")
    rd = lax.ppermute(od, "gx", swaps(gx, 1))
    rc = lax.ppermute(oc, "gx", swaps(gx, 0))
    ra = lax.ppermute(oa, GY, swaps(gy, 0))
    rb = lax.ppermute(ob, GY, swaps(gy, 1))
    return rb, rc, rd, ra


def rounded_to(x):
    return lax.reduce_precision(x, 8, 7)


def four_sum(x, axes, low, high):
    count = lax.axis_size(axes)
    x = rounded_to(x)
    sent = x.astype(BF16)
    one, two, three = (
        lax.ppermute(sent, axes, [(i, i ^ bits) for i in range(count)]).astype(F32)
        for bits in (low, high, low + high)
    )
    return (one + three) + (x + two)


def summed(x):
    x = four_sum(x, ("gx", "core"), 1, 2)
    x = four_sum(x, "y1", 1, 2)
    x = four_sum(x, "y0", 1, 2)
    return four_sum(x, "gx", 2, 4)


def on_device(blocks, block_cols, live_blocks, send_rows, start, sketch):
    rows, slots, size, _ = blocks.shape
    rhs = start.shape[1]
    width = send_rows.shape[2]
    count = sketch.shape[0]
    vector = jax.ShapeDtypeStruct(start.shape, F32)
    rounded = jax.ShapeDtypeStruct(start.shape, BF16)
    message = jax.ShapeDtypeStruct((width, rhs, size), BF16)
    part = jax.ShapeDtypeStruct((rhs, count), F32)
    src = pltpu.VMEM((rows + 4 * width + 1, rhs, size), BF16)
    flops = 2 * rows * slots * rhs * size * size
    sketch_flops = 6 * rows * rhs * size * count

    v0, send, x, *messages = call(
        first_kernel,
        "first",
        [HBM] * 2,
        [vector, jax.ShapeDtypeStruct(send_rows.shape, jnp.int32), rounded] + [message] * 4,
        [pltpu.SMEM(send_rows.shape, jnp.int32), pltpu.SemaphoreType.DMA((3,))],
        flops=1 << 20,
        nbytes=1 << 20,
    )(in_hbm(send_rows), in_hbm(start))
    received = exchange(messages)
    here, cols, live, high, low, w0 = call(
        prepare_kernel,
        "prepare",
        [HBM] * 4 + [VMEM],
        [
            jax.ShapeDtypeStruct(blocks.shape, BF16),
            jax.ShapeDtypeStruct(block_cols.shape, jnp.int32),
            jax.ShapeDtypeStruct(live_blocks.shape, jnp.int32),
            rounded,
            rounded,
            part,
        ],
        [pltpu.VMEM(sketch.shape, F32), pltpu.SemaphoreType.DMA((rows + 3,))],
        flops=sketch_flops,
        nbytes=blocks.size * 2,
    )(in_hbm(blocks), in_hbm(sketch), in_hbm(block_cols), in_hbm(live_blocks), v0)

    def step(x, received, *earlier):
        inputs = (cols, live, send, x, *received, here)

        def kernel(*refs):
            step_kernel(*refs[: len(inputs)], *refs[len(inputs) + len(earlier) :])

        return call(
            kernel,
            "step",
            [SMEM] * 3 + [VMEM] * (6 + len(earlier)),
            [vector, rounded] + [message] * 4,
            [src],
            flops=flops,
            nbytes=blocks.size * 2,
        )(*inputs, *earlier)

    sketch_of = call(sketch_kernel, "sketch", [VMEM] * 3, [part], flops=sketch_flops, nbytes=1 << 20)
    v1, x, *messages = step(x, received)
    received = exchange(messages)
    (w1,) = sketch_of(v1, high, low)
    half = rows // 2
    table = jax.ShapeDtypeStruct((src.shape[0], count, size), F32)

    def spread(name, low_row, high_row, extra):
        return call(
            lambda *refs: spread_kernel(low_row, high_row, *refs),
            name,
            [SMEM] * 2 + [VMEM] * (2 + extra),
            [table],
            flops=flops,
            nbytes=blocks.size,
        )

    (z,) = spread("spread", 0, half, 0)(cols, live, high, here)
    v2, x, *messages = step(x, received, z, w1)
    received = exchange(messages)
    (w2,) = sketch_of(v2, high, low)
    (z,) = spread("respread", half, rows, 1)(cols, live, high, here, z)
    half_table = jax.ShapeDtypeStruct((4 * width, count, size), BF16)
    own, z_high, z_low = call(
        own_kernel, "own", [VMEM] * 2, [part] + [half_table] * 2, flops=sketch_flops, nbytes=1 << 20
    )(x, z)
    (w,) = call(
        gather_kernel,
        "gather",
        [VMEM] * 10,
        [jax.ShapeDtypeStruct((2, rhs, 2 * count), F32)],
        flops=sketch_flops,
        nbytes=1 << 20,
    )(*received, z_high, z_low, w0, w1, w2, own)
    (v3,) = call(
        last_kernel,
        "last",
        [SMEM] * 2 + [VMEM] * 6,
        [vector],
        [src],
        flops=flops,
        nbytes=blocks.size * 2,
    )(cols, live, x, *received, here)
    w = summed(w)
    basis, factor = call(
        final_kernel,
        "final",
        [VMEM] * 5,
        [
            jax.ShapeDtypeStruct((STEPS + 1, *start.shape), F32),
            jax.ShapeDtypeStruct((STEPS + 1, STEPS + 1, rhs), F32),
        ],
        [
            pltpu.VMEM((STEPS + 1, *start.shape), F32),
            pltpu.VMEM((STEPS + 1, STEPS + 1, rhs), F32),
            pltpu.SemaphoreType.DMA((STEPS + 2,)),
        ],
        flops=1 << 22,
        nbytes=1 << 22,
        out_specs=[pl.BlockSpec(memory_space=pl.ANY)] * 2,
    )(v0, v1, v2, v3, w)
    return basis, factor


def solution(mesh):
    split = Mesh(mesh.devices.reshape(mesh.shape["gx"], 4, 4, 2), GX_GY)
    return jax.shard_map(
        on_device,
        mesh=split,
        in_specs=(
            P(GX_GY, None, None, None),
            P(GX_GY, None),
            P(GX_GY),
            P(GX_GY, None, None),
            P(GX_GY, None, None),
            P(None, GX_GY, None),
        ),
        out_specs=(P(None, GX_GY, None, None), P()),
        check_vma=False,
    )
```
